32 devices in a mesh: rep: 2 (over z, core), dp: 16 (over x, y).
Axes of the slice: x: 4, y: 4, z: 1, core: 2. Of those that a mesh axis runs over, the one named last changes fastest.
The devices are a block of a 4x4x8 slice.
Arguments:
- x: bfloat16 [32, 2048, 896], P(('rep', 'dp')), parts along dimension 0
- dy: bfloat16 [32, 2048, 896], P(('rep', 'dp')), parts along dimension 0
- w_gate: bfloat16 [2, 896, 3584], replicated
- w_up: bfloat16 [2, 896, 3584], replicated
- w_down: bfloat16 [2, 3584, 896], replicated
- m_w_gate: float32 [2, 896, 3584], P(None, 'dp')
- m_w_up: float32 [2, 896, 3584], P(None, 'dp')
- m_w_down: float32 [2, 3584, 896], P(None, 'dp')
- v_w_gate: float32 [2, 896, 3584], P(None, 'dp')
- v_w_up: float32 [2, 896, 3584], P(None, 'dp')
- v_w_down: float32 [2, 3584, 896], P(None, 'dp')
Outputs:
- output 1: bfloat16 [4, 896, 3584], P('rep'), parts along dimension 0
- output 2: bfloat16 [4, 896, 3584], P('rep'), parts along dimension 0
- output 3: bfloat16 [4, 3584, 896], P('rep'), parts along dimension 0
- output 4: float32 [4, 896, 3584], P('rep', 'dp'), parts along dimension 0
- output 5: float32 [4, 896, 3584], P('rep', 'dp'), parts along dimension 0
- output 6: float32 [4, 3584, 896], P('rep', 'dp'), parts along dimension 0
- output 7: float32 [4, 896, 3584], P('rep', 'dp'), parts along dimension 0
- output 8: float32 [4, 896, 3584], P('rep', 'dp'), parts along dimension 0
- output 9: float32 [4, 3584, 896], P('rep', 'dp'), parts along dimension 0
There are 2 independent parts. The reference program is written for one: setup_inputs(seed, part) draws one part's arguments, and reference() takes and returns one part's arrays. A program takes and returns all parts, laid end to end along the dimension named above; an argument that names none is the same for every part.
All inputs are finite; a program needn't handle non-finite values.
Results may differ from the reference program's by a relative error of at most 0.022.
Values are sent between devices in bfloat16 or wider.
A program may use at most 768 MiB of HBM per device.

```python
import jax
import jax.numpy as jnp
from jax import lax

SEQUENCES = 16
TOKENS = 2048
D = 896
FF = 3584
LAYERS = 2
NAMES = ("w_gate", "w_up", "w_down")
SHAPES = {"w_gate": (LAYERS, D, FF), "w_up": (LAYERS, D, FF), "w_down": (LAYERS, FF, D)}


def bump(key, n, height):
    away = (jnp.arange(n, dtype=jnp.int32) - jax.random.randint(key, (), 0, n, jnp.int32)) % n
    return jnp.where(away < n // 8, height, 1.0)


def together(key, own, strength):
    shared = jax.random.normal(key, own.shape[1:], jnp.float32)
    return (own + strength * shared) * lax.rsqrt(1 + strength * strength)


def setup_inputs(seed: int = 0, part: int = 0) -> dict:
    kx, kdy, ka, kb, kz, kf, kh, kl, *keys = jax.random.split(jax.random.key(seed), 8 + 3 * len(NAMES))
    kx, kdy, ka, kb = (jax.random.fold_in(k, part) for k in (kx, kdy, ka, kb))
    kw, km, kv = (keys[i::3] for i in range(3))
    shape = (SEQUENCES, TOKENS, D)
    much_x, much_dy = jax.random.uniform(kz, (2,), jnp.float32, 0.0, 1.0)
    loud = 2.0 ** jax.random.uniform(jax.random.fold_in(kz, 1), (), jnp.float32, -1.0, 2.0)
    layers = 2.0 ** jax.random.uniform(kl, (LAYERS, 1, 1), jnp.float32, -1.0, 1.0)
    x = together(ka, jax.random.normal(kx, shape, jnp.float32), much_x) * bump(kf, D, 4.0)
    dy = together(kb, jax.random.normal(kdy, shape, jnp.float32), much_dy)
    drawn = {"x": x.astype(jnp.bfloat16), "dy": (loud * dy * (SEQUENCES * TOKENS) ** -0.5).astype(jnp.bfloat16)}
    for key, name in zip(kw, NAMES, strict=True):
        w = jax.random.normal(key, SHAPES[name], jnp.float32) * SHAPES[name][1] ** -0.5
        drawn[name] = (w * {"w_gate": 1.0, "w_up": bump(kh, FF, 4.0), "w_down": layers}[name]).astype(jnp.bfloat16)
    for key, name in zip(km, NAMES, strict=True):
        drawn[f"m_{name}"] = 0.1 * jax.random.normal(key, SHAPES[name], jnp.float32)
    for key, name in zip(kv, NAMES, strict=True):
        drawn[f"v_{name}"] = jax.random.uniform(key, SHAPES[name], jnp.float32, 0.005, 0.015)
    return drawn


def matmul(a, w):
    return jnp.dot(a, w, preferred_element_type=jnp.float32).astype(jnp.bfloat16)


def normed(h):
    wide = h.astype(jnp.float32)
    scale = lax.rsqrt(jnp.mean(wide**2, -1, keepdims=True) + 1e-6)
    return (wide * scale).astype(jnp.bfloat16)


def layer(h, w):
    a = normed(h)
    gate = jnp.dot(a, w["w_gate"], preferred_element_type=jnp.float32)
    up = jnp.dot(a, w["w_up"], preferred_element_type=jnp.float32)
    return h + matmul((jax.nn.silu(gate) * up).astype(jnp.bfloat16), w["w_down"])


def adamw(w, m, v, g):
    m = 0.9 * m + 0.1 * g
    v = 0.95 * v + 0.05 * g * g
    step = m * lax.rsqrt(v + 1e-8) + 0.1 * w
    return (w - 0.02 * step).astype(jnp.bfloat16), m, v


def stack(weights, h):
    return lax.scan(lambda h, w: (layer(h, w), None), h, weights)[0]


def reference(x, dy, w_gate, w_up, w_down, m_w_gate, m_w_up, m_w_down, v_w_gate, v_w_up, v_w_down):
    weights = dict(zip(NAMES, (w_gate, w_up, w_down), strict=True))

    def take(so_far, sequence):
        h, by_y = sequence
        _, back = jax.vjp(lambda w: stack(w, h), weights)
        return jax.tree.map(lambda total, term: total + term.astype(jnp.float32), so_far, back(by_y)[0]), None

    none_yet = {name: jnp.zeros(w.shape, jnp.float32) for name, w in weights.items()}
    by_weights, _ = lax.scan(take, none_yet, (x, dy))
    gradients = [by_weights[name].astype(jnp.bfloat16).astype(jnp.float32) for name in NAMES]
    new = [
        adamw(w.astype(jnp.float32), m, v, g)
        for w, m, v, g in zip((w_gate, w_up, w_down), (m_w_gate, m_w_up, m_w_down), (v_w_gate, v_w_up, v_w_down), gradients, strict=True)
    ]
    return tuple(one[which] for which in range(3) for one in new)
```

```python
import functools
import math

import jax
import jax.numpy as jnp
from jax import lax
from jax.experimental import pallas as pl
from jax.experimental.pallas import tpu as pltpu
from jax.sharding import PartitionSpec as P

BLOCK = 256
CHUNKS = 4
LANES = 128
MESH = pl.DeviceIdType.MESH
F32, BF16 = jnp.float32, jnp.bfloat16


def dot(a, b, contract=((1,), (0,))):
    return lax.dot_general(a, b, (contract, ((), ())), preferred_element_type=F32)


def normed(h):
    wide = h.astype(F32)
    scale = lax.rsqrt(jnp.mean(wide**2, -1, keepdims=True) + 1e-6)
    return (wide * scale).astype(BF16)


def adamw(w, m, v, g):
    m = 0.9 * m + 0.1 * g
    v = 0.95 * v + 0.05 * g * g
    step = m * lax.rsqrt(v + 1e-8) + 0.1 * w
    return (w - 0.02 * step).astype(BF16), m, v


def whole(shape):
    return pl.BlockSpec(shape, lambda *_: (0,) * len(shape), pipeline_mode=pl.Buffered(1))


def forward_kernel(x_ref, wg_ref, wu_ref, wd_ref, h_ref, a_ref, acc_ref):
    tokens = x_ref.shape[0]
    chunks, CHUNK = CHUNKS, tokens // CHUNKS
    f = pl.program_id(0)

    @pl.when(f == 0)
    def _():
        @pl.loop(0, chunks)
        def _(c):
            rows = pl.ds(c * CHUNK, CHUNK)
            a_ref[rows] = normed(x_ref[rows])
            acc_ref[rows] = jnp.zeros((CHUNK, x_ref.shape[1]), F32)

    wg, wu, wd = wg_ref[0], wu_ref[0], wd_ref[0]
    for c in range(chunks):
        rows = pl.ds(c * CHUNK, CHUNK)
        a = a_ref[rows]
        gate, up = dot(a, wg), dot(a, wu)
        hidden = (gate * jax.nn.sigmoid(gate) * up).astype(BF16)
        acc_ref[rows] += dot(hidden, wd)

    @pl.when(f == pl.num_programs(0) - 1)
    def _():
        @pl.loop(0, chunks)
        def _(c):
            rows = pl.ds(c * CHUNK, CHUNK)
            h_ref[rows] = x_ref[rows] + acc_ref[rows].astype(BF16)


def forward(x, wg, wu, wd, layer):
    tokens, d = x.shape
    ff = wg.shape[2]
    cost = 6 * tokens * d * ff
    return pl.pallas_call(
        forward_kernel,
        grid=(ff // BLOCK,),
        in_specs=[
            whole((tokens, d)),
            pl.BlockSpec((1, d, BLOCK), lambda f: (layer, 0, f)),
            pl.BlockSpec((1, d, BLOCK), lambda f: (layer, 0, f)),
            pl.BlockSpec((1, BLOCK, d), lambda f: (layer, f, 0)),
        ],
        out_specs=whole((tokens, d)),
        out_shape=jax.ShapeDtypeStruct((tokens, d), BF16),
        scratch_shapes=[pltpu.VMEM((tokens, d), BF16), pltpu.VMEM((tokens, d), F32)],
        cost_estimate=pl.CostEstimate(flops=cost, bytes_accessed=3 * 2 * d * ff, transcendentals=tokens * ff),
        compiler_params=pltpu.CompilerParams(vmem_limit_bytes=60 * 2**20),
        name="forward",
    )(x, wg, wu, wd)


class Ring:
    def __init__(self, side):
        me = lax.axis_index("dp")
        self.side = side
        self.at = (lax.div(me, side), lax.rem(me, side))

    def place(self, axis, offset):
        return lax.rem(self.at[axis] + offset + self.side, self.side)

    def device(self, axis, offset):
        there = [self.at[0], self.at[1]]
        there[axis] = self.place(axis, offset)
        return {"dp": there[0] * self.side + there[1]}

    def meet(self):
        barrier = pltpu.get_barrier_semaphore()
        for axis in range(2):
            for offset in (1, -1):
                pl.semaphore_signal(barrier, inc=1, device_id=self.device(axis, offset), device_id_type=MESH)
        pl.semaphore_wait(barrier, 4)


class Scatter:
    def __init__(self, ring, axis, terms, far, near, sems):
        self.ring, self.axis, self.terms, self.far, self.near, self.sems = ring, axis, terms, far, near, sems

    def copy(self, src, dst, number, offset):
        return pltpu.make_async_remote_copy(
            src_ref=src,
            dst_ref=dst,
            send_sem=self.sems.at[0, number],
            recv_sem=self.sems.at[1, number],
            device_id=self.ring.device(self.axis, offset),
            device_id_type=MESH,
        )

    def first(self, half):
        opposite = self.ring.place(self.axis, 2)
        return self.copy(self.terms.at[opposite, half], self.far.at[half], half, 1 - 2 * half)

    def second(self, side):
        offset = 1 - 2 * side
        return self.copy(self.terms.at[self.ring.place(self.axis, offset)], self.near.at[side], 2 + side, offset)

    def relay(self, own=None):
        for side in range(2):
            self.first(side).wait()
            place = self.ring.place(self.axis, 1 - 2 * side)
            term = self.terms[place, side].astype(F32) if own is None else own(place, side)
            self.terms[place, side] = (term + self.far[side].astype(F32)).astype(BF16)
        for side in range(2):
            self.second(side).start()

    def arrive(self):
        for side in range(2):
            self.second(side).wait()

    def received(self, half):
        return self.near[0, half].astype(F32) + self.near[1, half].astype(F32)


def backward_kernel(side, wanted, h_hbm, dy_ref, *refs):
    wg_refs, wu_refs, wd_refs, refs = refs[:side], refs[side : 2 * side], refs[2 * side : 3 * side], refs[3 * side :]
    gg_ref, gu_ref, gd_ref, h_ref, refs = *refs[:4], refs[4:]
    a_ref, at_ref, dyt_ref, hid_ref, dgate_ref, dup_ref, held_ref, local_sem, refs = *refs[:8], refs[8:]
    ga, gb, gd, ra, rb, rd, na, nb, nd, sa, sb, sd, refs = *refs[:12], refs[12:]
    ha, hb, hd, ra2, rb2, rd2, na2, nb2, nd2, sems, refs = *refs[:10], refs[10:]
    if wanted:
        da_ref = refs[0]
    tokens, d = dy_ref.shape
    size = tokens // CHUNKS
    t, steps = pl.program_id(0), pl.num_programs(0) - 1
    rows = gg_ref.shape[0]
    ring = Ring(side)
    half_d = hd.shape[2]
    first_a, first_b, first_d = (
        Scatter(ring, axis, g, r, n, sems.at[i]) for i, (axis, g, r, n) in enumerate(((0, ga, ra, na), (1, gb, rb, nb), (0, gd, rd, nd)))
    )
    second_a, second_b, second_d = (
        Scatter(ring, axis, g, r, n, sems.at[3 + i])
        for i, (axis, g, r, n) in enumerate(((1, ha, ra2, na2), (0, hb, rb2, nb2), (1, hd, rd2, nd2)))
    )

    @pl.when(t == 0)
    def _():
        ring.meet()
        copy = pltpu.make_async_copy(h_hbm, h_ref, local_sem)
        copy.start()
        copy.wait()
        for c in range(CHUNKS):
            part = pl.ds(c * size, size)
            a = normed(h_ref[part])
            a_ref[part] = a
            at_ref[:, part] = a.T
            dyt_ref[:, part] = dy_ref[part].T
            if wanted:
                da_ref[part] = jnp.zeros((size, d), F32)

    def joined(refs, axis):
        return jnp.concatenate([ref[0] for ref in refs], axis)

    def chunk(c):
        wg, wu, wd = joined(wg_refs, 1), joined(wu_refs, 1), joined(wd_refs, 0)
        part = pl.ds(c * size, size)
        a = a_ref[part]
        gate, up = dot(a, wg), dot(a, wu)
        dhid = dot(dy_ref[part], wd, ((1,), (1,))).astype(BF16).astype(F32)
        s = jax.nn.sigmoid(gate)
        silu = gate * s
        hid_ref[part] = (silu * up).astype(BF16)
        dup = (dhid * silu).astype(BF16)
        dgate = (dhid * up * (s * (1 + gate * (1 - s)))).astype(BF16)
        dup_ref[part] = dup
        dgate_ref[part] = dgate
        if wanted:
            da_ref[part] += dot(dgate, wg, ((1,), (1,))) + dot(dup, wu, ((1,), (1,)))

    def put(g, half):
        for place in range(side):
            ga[place, half] = g[side * rows * place : side * rows * (place + 1), :LANES].astype(BF16)
            mine = [g[rows * (side * x + place) : rows * (side * x + place + 1), LANES:] for x in range(side)]
            gb[place, half] = jnp.concatenate(mine, 0).astype(BF16)

    computing, summing = t < steps, t > 0

    @pl.when(computing)
    def _():
        chunk(0)
        chunk(1)

    @pl.when(summing)
    def _():
        for one in (first_a, first_b, first_d):
            one.relay()

    @pl.when(computing)
    def _():
        chunk(2)
        chunk(3)
        g = dot(dyt_ref[...], hid_ref[...]).T.astype(BF16)
        held_ref[...] = g.reshape(held_ref.shape)

    @pl.when(summing)
    def _():
        for one in (first_a, first_b, first_d):
            one.arrive()
        for one, two, total in ((first_a, second_a, sa), (first_b, second_b, sb)):
            place = ring.place(one.axis, 0)
            for half in range(2):
                value = one.terms[place, half].astype(F32) + one.received(half)
                total[half] = value
                for p in range(side):
                    two.terms[p, half] = value[rows * p : rows * (p + 1)].astype(BF16)
                two.first(half).start()
        place = ring.place(0, 0)
        for half in range(2):
            value = gd[place, half].astype(F32) + first_d.received(half)
            count = value.shape[0]
            sd[pl.ds(pl.multiple_of((2 * (t - 1) + half) * count, count), count)] = value

    @pl.when(computing)
    def _():
        gd[...] = held_ref[...]
        for half in range(2):
            first_d.first(half).start()
        g = dot(at_ref[...], dgate_ref[...])
        put(g, 0)
        first_a.first(0).start()
        first_b.first(0).start()

    def own(total):
        return lambda place, half: total[half, pl.ds(pl.multiple_of(place * rows, 8), rows)]

    @pl.when(summing)
    def _():
        second_a.relay(own(sa))
        second_b.relay(own(sb))

    @pl.when(computing)
    def _():
        g = dot(at_ref[...], dup_ref[...])
        put(g, 1)
        first_a.first(1).start()
        first_b.first(1).start()

    @pl.when(summing)
    def _():
        second_a.arrive()
        second_b.arrive()
        for two, total, tile in ((second_a, sa, 0), (second_b, sb, 1)):
            place = ring.place(two.axis, 0)
            for half, out in enumerate((gg_ref, gu_ref)):
                value = (own(total)(place, half) + two.received(half)).astype(BF16)
                for j in range(value.shape[1] // LANES):
                    lane = pl.multiple_of((t - 1 + steps * (tile + j)) * LANES, LANES)
                    out[:, pl.ds(lane, LANES)] = value[:, j * LANES : (j + 1) * LANES]

    if wanted:

        @pl.when(t == steps - 1)
        def _():
            for c in range(CHUNKS):
                part = pl.ds(c * size, size)
                wide = h_ref[part].astype(F32)
                by_a = da_ref[part].astype(BF16).astype(F32)
                scale = lax.rsqrt(jnp.mean(wide**2, -1, keepdims=True) + 1e-6)
                along = jnp.mean(by_a * wide, -1, keepdims=True)
                by_h = by_a * scale - wide * (along * scale * scale * scale)
                h_ref[part] = dy_ref[part] + by_h.astype(BF16)

    @pl.when(t == steps)
    def _():
        def mine(place, half):
            return sd[pl.ds(pl.multiple_of((2 * place + half) * half_d, 8), half_d)]

        for p in range(side):
            for half in range(2):
                hd[p, half] = mine(p, half).astype(BF16)
        for half in range(2):
            second_d.first(half).start()
        second_d.relay(mine)
        second_d.arrive()
        place = ring.place(1, 0)
        for half in range(2):
            gd_ref[half * half_d : (half + 1) * half_d] = (mine(place, half) + second_d.received(half)).astype(BF16)


def backward(side, h, dy, wg, wu, wd, layer, wanted):
    tokens, d = h.shape
    ff = wg.shape[2]
    tiles = ff // LANES
    steps = tiles // side
    rows, down_rows = d // side**2, ff // side**2
    width = side * LANES

    def tile(j):
        return lambda t: jnp.minimum(t, steps - 1) + steps * j

    across = [pl.BlockSpec((1, d, LANES), lambda t, j=j: (layer, 0, tile(j)(t))) for j in range(side)]
    down = [pl.BlockSpec((1, LANES, d), lambda t, j=j: (layer, tile(j)(t), 0)) for j in range(side)]
    shapes = [(side, 2, side * rows, LANES), (side, 2, side * rows, width - LANES), (side, 2, LANES // 2, d)]
    shapes2 = [(side, 2, rows, LANES), (side, 2, rows, width - LANES), (side, 2, down_rows // 2, d)]

    def buffers(shapes):
        terms = [pltpu.VMEM(s, BF16) for s in shapes]
        far = [pltpu.VMEM(s[1:], BF16) for s in shapes]
        near = [pltpu.VMEM((2, *s[1:]), BF16) for s in shapes]
        return terms + far + near

    totals = [
        pltpu.VMEM((2, side * rows, LANES), F32),
        pltpu.VMEM((2, side * rows, width - LANES), F32),
        pltpu.VMEM((side * down_rows, d), F32),
    ]
    scratch = [
        pltpu.VMEM((tokens, d), BF16),
        pltpu.VMEM((d, tokens), BF16),
        pltpu.VMEM((d, tokens), BF16),
        pltpu.VMEM((tokens, width), BF16),
        pltpu.VMEM((tokens, width), BF16),
        pltpu.VMEM((tokens, width), BF16),
        pltpu.VMEM(shapes[2], BF16),
        pltpu.SemaphoreType.DMA,
        *buffers(shapes),
        *totals,
        *buffers(shapes2),
        pltpu.SemaphoreType.DMA((6, 2, 4)),
    ]
    out_specs = [whole((rows, ff)), whole((rows, ff)), whole((down_rows, d)), whole((tokens, d))]
    out_shape = [jax.ShapeDtypeStruct(s, BF16) for s in ((rows, ff), (rows, ff), (down_rows, d), (tokens, d))]
    if wanted:
        scratch.append(pltpu.VMEM((tokens, d), F32))
    return pl.pallas_call(
        functools.partial(backward_kernel, side, wanted),
        grid=(steps + 1,),
        in_specs=[pl.BlockSpec(memory_space=pl.ANY), whole((tokens, d)), *across, *across, *down],
        out_specs=out_specs,
        out_shape=out_shape,
        scratch_shapes=scratch,
        cost_estimate=pl.CostEstimate(
            flops=2 * tokens * d * ff * (8 if wanted else 6), bytes_accessed=6 * 2 * d * ff, transcendentals=tokens * ff
        ),
        compiler_params=pltpu.CompilerParams(vmem_limit_bytes=63 * 2**20, collective_id=1 + layer, has_side_effects=True),
        name=f"backward_{layer}",
    )(h, dy, *[wg] * side, *[wu] * side, *[wd] * side)


def gather_kernel(side, *refs):
    count = len(refs) // 2 - 1
    shards, outs, (sems, local_sems) = refs[:count], refs[count : 2 * count], refs[2 * count :]
    ring = Ring(side)
    ring.meet()
    units = [(i, n) for n in reversed(range(shards[0].shape[0])) for i in range(count)]
    me = ring.at[0] * side + ring.at[1]

    def rows_of(i, first, many=1):
        rows = shards[i].shape[1]
        return pl.ds(pl.multiple_of(first * rows, 8), many * rows)

    def halves(ref, i, n, first, many, half):
        rows, columns = shards[i].shape[1:]
        if columns % (2 * LANES) == 0:
            return ref.at[n, rows_of(i, first, many), pl.ds(half * (columns // 2), columns // 2)]
        length = many * rows // 2
        return ref.at[n, pl.ds(pl.multiple_of(first * rows + half * length, 8), length)]

    class Phase:
        def __init__(self, number, i, n, axis, first, many, src):
            self.number, self.i, self.n, self.axis, self.first, self.many, self.src = number, i, n, axis, first, many, src

        def copy(self, src, dst, which, offset):
            return pltpu.make_async_remote_copy(
                src_ref=src,
                dst_ref=dst,
                send_sem=sems.at[0, self.number, which],
                recv_sem=sems.at[1, self.number, which],
                device_id=ring.device(self.axis, offset),
                device_id_type=MESH,
            )

        def near(self, side):
            dst = outs[self.i].at[self.n, rows_of(self.i, self.first(0), self.many)]
            return self.copy(dst if self.src is None else self.src, dst, side, 1 - 2 * side)

        def far(self, side):
            offset = 1 - 2 * side
            part = halves(outs[self.i], self.i, self.n, self.first(-offset), self.many, side)
            return self.copy(part, part, 2 + side, offset)

        def start(self):
            for side in range(2):
                self.near(side).start()

        def relay(self):
            for side in range(2):
                self.near(side).wait_recv()
                self.far(side).start()

        def arrive(self):
            for side in range(2):
                self.far(side).wait_recv()

        def finish(self):
            for side in range(2):
                self.near(side).wait_send()
                self.far(side).wait_send()

    one, two, number = {}, {}, 0
    for i, n in units:
        own = shards[i].at[n]
        if n % 2:
            one[i, n] = Phase(number, i, n, 1, lambda o: ring.at[0] * side + ring.place(1, o), 1, own)
            two[i, n] = [Phase(number + 1, i, n, 0, lambda o: ring.place(0, o) * side, side, None)]
        else:
            one[i, n] = Phase(number, i, n, 0, lambda o: ring.place(0, o) * side + ring.at[1], 1, own)
            two[i, n] = [
                Phase(number + 1 + k, i, n, 1, lambda o, k=k: k * side + ring.place(1, o), 1, None) for k in range(side)
            ]
        number += 1 + len(two[i, n])

    def local(i, n):
        return pltpu.make_async_copy(shards[i].at[n], outs[i].at[n, rows_of(i, me)], local_sems.at[i, n])

    for unit in units:
        one[unit].start()
        local(*unit).start()
    for unit in units:
        one[unit].relay()
    for unit in units:
        one[unit].arrive()
        local(*unit).wait()
        for phase in two[unit]:
            phase.start()
    for unit in units:
        for phase in two[unit]:
            phase.relay()
    for unit in units:
        for phase in two[unit]:
            phase.arrive()
    for unit in units:
        for phase in (one[unit], *two[unit]):
            phase.finish()


def gather(side, shards):
    layers = shards[0].shape[0]
    phases = len(shards) * sum(2 if n % 2 else 1 + side for n in range(layers))
    return pl.pallas_call(
        functools.partial(gather_kernel, side),
        in_specs=[pl.BlockSpec(memory_space=pltpu.VMEM)] * len(shards),
        out_specs=[pl.BlockSpec(memory_space=pl.ANY)] * len(shards),
        out_shape=[jax.ShapeDtypeStruct((layers, s.shape[1] * side**2, s.shape[2]), s.dtype) for s in shards],
        scratch_shapes=[
            pltpu.SemaphoreType.DMA((2, phases, 4)),
            pltpu.SemaphoreType.DMA((len(shards), layers)),
        ],
        compiler_params=pltpu.CompilerParams(vmem_limit_bytes=60 * 2**20, collective_id=0, has_side_effects=True),
        name="gather",
    )(*shards)


def solution(mesh):
    side = math.isqrt(mesh.shape["dp"])

    def step(x, dy, *arrays):
        weights, ms, vs = (arrays[i : i + 3] for i in (0, 3, 6))
        x, dy = x[0], dy[0]
        layers = weights[0].shape[0]
        me = lax.axis_index("dp")

        states = [x]
        for n in range(layers - 1):
            states.append(forward(states[-1], *weights, n))

        grads = [None] * layers
        for n in reversed(range(layers)):
            *grads[n], dy = backward(side, states[n], dy, *weights, n, n > 0)
        new = []
        for which in range(3):
            w, m, v = weights[which], ms[which], vs[which]
            rows = m.shape[1]
            mine = lax.dynamic_slice_in_dim(w, me * rows, rows, 1)
            g = jnp.stack([grads[n][which] for n in range(layers)])
            new.append(adamw(mine.astype(F32), m, v, g.astype(F32)))
        gathered = gather(side, [one[0] for one in new])
        return (*gathered, *(one[1] for one in new), *(one[2] for one in new))

    tokens, row = P(("rep", "dp"), None, None), P(None, "dp", None)
    return jax.shard_map(
        step,
        mesh=mesh,
        in_specs=(tokens,) * 2 + (P(),) * 3 + (row,) * 6,
        out_specs=(P("rep", None, None),) * 3 + (P("rep", "dp", None),) * 6,
        check_vma=False,
    )
```

```python
import functools
import math

import jax
import jax.numpy as jnp
from jax import lax
from jax.experimental import pallas as pl
from jax.experimental.pallas import tpu as pltpu
from jax.sharding import PartitionSpec as P

BLOCK = 256
CHUNKS = 4
LANES = 128
MESH = pl.DeviceIdType.MESH
F32, BF16 = jnp.float32, jnp.bfloat16


def dot(a, b, contract=((1,), (0,))):
    return lax.dot_general(a, b, (contract, ((), ())), preferred_element_type=F32)


def normed(h):
    wide = h.astype(F32)
    scale = lax.rsqrt(jnp.mean(wide**2, -1, keepdims=True) + 1e-6)
    return (wide * scale).astype(BF16)


def adamw(w, m, v, g):
    m = 0.9 * m + 0.1 * g
    v = 0.95 * v + 0.05 * g * g
    step = m * lax.rsqrt(v + 1e-8) + 0.1 * w
    return (w - 0.02 * step).astype(BF16), m, v


def whole(shape):
    return pl.BlockSpec(shape, lambda *_: (0,) * len(shape), pipeline_mode=pl.Buffered(1))


def forward_kernel(x_ref, wg_ref, wu_ref, wd_ref, h_ref, a_ref, acc_ref):
    tokens = x_ref.shape[0]
    chunks, CHUNK = CHUNKS, tokens // CHUNKS
    f = pl.program_id(0)

    @pl.when(f == 0)
    def _():
        @pl.loop(0, chunks)
        def _(c):
            rows = pl.ds(c * CHUNK, CHUNK)
            a_ref[rows] = normed(x_ref[rows])
            acc_ref[rows] = jnp.zeros((CHUNK, x_ref.shape[1]), F32)

    wg, wu, wd = wg_ref[0], wu_ref[0], wd_ref[0]
    for c in range(chunks):
        rows = pl.ds(c * CHUNK, CHUNK)
        a = a_ref[rows]
        gate, up = dot(a, wg), dot(a, wu)
        hidden = (gate * jax.nn.sigmoid(gate) * up).astype(BF16)
        acc_ref[rows] += dot(hidden, wd)

    @pl.when(f == pl.num_programs(0) - 1)
    def _():
        @pl.loop(0, chunks)
        def _(c):
            rows = pl.ds(c * CHUNK, CHUNK)
            h_ref[rows] = x_ref[rows] + acc_ref[rows].astype(BF16)


def forward(x, wg, wu, wd, layer):
    tokens, d = x.shape
    ff = wg.shape[2]
    cost = 6 * tokens * d * ff
    return pl.pallas_call(
        forward_kernel,
        grid=(ff // BLOCK,),
        in_specs=[
            whole((tokens, d)),
            pl.BlockSpec((1, d, BLOCK), lambda f: (layer, 0, f)),
            pl.BlockSpec((1, d, BLOCK), lambda f: (layer, 0, f)),
            pl.BlockSpec((1, BLOCK, d), lambda f: (layer, f, 0)),
        ],
        out_specs=whole((tokens, d)),
        out_shape=jax.ShapeDtypeStruct((tokens, d), BF16),
        scratch_shapes=[pltpu.VMEM((tokens, d), BF16), pltpu.VMEM((tokens, d), F32)],
        cost_estimate=pl.CostEstimate(flops=cost, bytes_accessed=3 * 2 * d * ff, transcendentals=tokens * ff),
        compiler_params=pltpu.CompilerParams(vmem_limit_bytes=60 * 2**20),
        name="forward",
    )(x, wg, wu, wd)


class Ring:
    def __init__(self, side):
        me = lax.axis_index("dp")
        self.side = side
        self.at = (lax.div(me, side), lax.rem(me, side))

    def place(self, axis, offset):
        return lax.rem(self.at[axis] + offset + self.side, self.side)

    def device(self, axis, offset):
        there = [self.at[0], self.at[1]]
        there[axis] = self.place(axis, offset)
        return {"dp": there[0] * self.side + there[1]}

    def meet(self):
        barrier = pltpu.get_barrier_semaphore()
        for axis in range(2):
            for offset in (1, -1):
                pl.semaphore_signal(barrier, inc=1, device_id=self.device(axis, offset), device_id_type=MESH)
        pl.semaphore_wait(barrier, 4)


class Scatter:
    def __init__(self, ring, axis, terms, far, near, sems):
        self.ring, self.axis, self.terms, self.far, self.near, self.sems = ring, axis, terms, far, near, sems

    def copy(self, src, dst, number, offset):
        return pltpu.make_async_remote_copy(
            src_ref=src,
            dst_ref=dst,
            send_sem=self.sems.at[0, number],
            recv_sem=self.sems.at[1, number],
            device_id=self.ring.device(self.axis, offset),
            device_id_type=MESH,
        )

    def first(self, half):
        opposite = self.ring.place(self.axis, 2)
        return self.copy(self.terms.at[opposite, half], self.far.at[half], half, 1 - 2 * half)

    def second(self, side):
        offset = 1 - 2 * side
        return self.copy(self.terms.at[self.ring.place(self.axis, offset)], self.near.at[side], 2 + side, offset)

    def relay(self, own=None):
        for side in range(2):
            self.first(side).wait()
            place = self.ring.place(self.axis, 1 - 2 * side)
            term = self.terms[place, side].astype(F32) if own is None else own(place, side)
            self.terms[place, side] = (term + self.far[side].astype(F32)).astype(BF16)
        for side in range(2):
            self.second(side).start()

    def arrive(self):
        for side in range(2):
            self.second(side).wait()

    def received(self, half):
        return self.near[0, half].astype(F32) + self.near[1, half].astype(F32)


class Piece:
    def __init__(self, ring, axis, src, block, part, sems, number):
        self.ring, self.axis, self.src, self.block, self.part, self.sems, self.number = ring, axis, src, block, part, sems, number

    def copy(self, src, dst, which, offset):
        return pltpu.make_async_remote_copy(
            src_ref=src,
            dst_ref=dst,
            send_sem=self.sems.at[0, self.number, which],
            recv_sem=self.sems.at[1, self.number, which],
            device_id=self.ring.device(self.axis, offset),
            device_id_type=MESH,
        )

    def near(self, side):
        return self.copy(self.block(0) if self.src is None else self.src, self.block(0), side, 1 - 2 * side)

    def far(self, side):
        offset = 1 - 2 * side
        return self.copy(self.part(-offset, side), self.part(-offset, side), 2 + side, offset)

    def start(self):
        for side in range(2):
            self.near(side).start()

    def relay(self):
        for side in range(2):
            self.near(side).wait_recv()
            self.far(side).start()

    def arrive(self):
        for side in range(2):
            self.far(side).wait_recv()

    def sent(self):
        for side in range(2):
            self.near(side).wait_send()
            self.far(side).wait_send()


class Gather:
    def __init__(self, ring, shards, outs, layer, sems, local_sems):
        self.ring, self.shards, self.outs, self.layer, self.local_sems = ring, shards, outs, layer, local_sems
        side = ring.side
        self.ones, self.pairs = [], []
        for i in range(3):
            pair = [[] for _ in range(side)]
            for half in range(2):
                axis = 1 - half
                unit = 2 * i + half

                def owner(offset, axis=axis):
                    at = [ring.at[0], ring.at[1]]
                    at[axis] = ring.place(axis, offset)
                    return at[0] * side + at[1]

                self.ones.append(self.piece(i, half, axis, owner, self.region(shards[i], i, 0, half), sems, unit))
                for k in range(side):

                    def owner(offset, axis=axis, k=k):
                        at = [k, k]
                        at[1 - axis] = ring.place(1 - axis, offset)
                        return at[0] * side + at[1]

                    pair[k].append(self.piece(i, half, 1 - axis, owner, None, sems, 6 + unit * side + k))
            self.pairs += pair

    def piece(self, i, half, axis, owner, src, sems, number):
        out = self.outs[i].at[self.layer]
        return Piece(
            self.ring,
            axis,
            src,
            lambda offset: self.region(out, i, owner(offset), half),
            lambda offset, part: self.region(out, i, owner(offset), half, part),
            sems,
            number,
        )

    def region(self, ref, i, owner, half, part=None):
        rows, columns = self.shards[i].shape
        share = 2 if part is None else 4
        which = half if part is None else 2 * half + part
        if columns % (4 * LANES) == 0:
            first = owner * rows
            return ref.at[pl.ds(pl.multiple_of(first, 8), rows), pl.ds(which * (columns // share), columns // share)]
        length = rows // share
        return ref.at[pl.ds(pl.multiple_of(owner * rows + which * length, 8), length)]

    def local(self, i):
        rows = self.shards[i].shape[0]
        me = self.ring.at[0] * self.ring.side + self.ring.at[1]
        out = self.outs[i].at[self.layer, pl.ds(pl.multiple_of(me * rows, 8), rows)]
        return pltpu.make_async_copy(self.shards[i], out, self.local_sems.at[i])

    def start(self):
        for one in self.ones:
            one.start()
        for i in range(3):
            self.local(i).start()

    def relay(self):
        for one in self.ones:
            one.relay()

    def arrive(self):
        for one in self.ones:
            one.arrive()
        for i in range(3):
            self.local(i).wait()

    def finish(self):
        for pair in self.pairs:
            for piece in pair:
                piece.arrive()
        for one in (*self.ones, *(piece for pair in self.pairs for piece in pair)):
            one.sent()


def backward_kernel(side, wanted, gathered, h_hbm, dy_ref, *refs):
    wg_refs, wu_refs, wd_refs, refs = refs[:side], refs[side : 2 * side], refs[2 * side : 3 * side], refs[3 * side :]
    if gathered is not None:
        shards, refs = refs[:3], refs[3:]
    gg_ref, gu_ref, gd_ref, *refs = refs
    if wanted:
        h_ref, *refs = refs
    if gathered is not None:
        outs, refs = refs[:3], refs[3:]
    a_ref, at_ref, dyt_ref, hid_ref, dgate_ref, dup_ref, held_ref, local_sem, refs = *refs[:8], refs[8:]
    ga, gb, gd, ra, rb, rd, na, nb, nd, sa, sb, sd, refs = *refs[:12], refs[12:]
    ha, hb, hd, ra2, rb2, rd2, na2, nb2, nd2, sems, refs = *refs[:10], refs[10:]
    if wanted:
        da_ref, *refs = refs
    else:
        h_ref, *refs = refs
    tokens, d = dy_ref.shape
    size = tokens // CHUNKS
    t, steps = pl.program_id(0), pl.num_programs(0) - 1
    rows = gg_ref.shape[0]
    ring = Ring(side)
    half_d = hd.shape[2]
    first_a, first_b, first_d = (
        Scatter(ring, axis, g, r, n, sems.at[i]) for i, (axis, g, r, n) in enumerate(((0, ga, ra, na), (1, gb, rb, nb), (0, gd, rd, nd)))
    )
    second_a, second_b, second_d = (
        Scatter(ring, axis, g, r, n, sems.at[3 + i])
        for i, (axis, g, r, n) in enumerate(((1, ha, ra2, na2), (0, hb, rb2, nb2), (1, hd, rd2, nd2)))
    )

    if gathered is not None:
        others = Gather(ring, shards, outs, gathered, *refs)

    def beside(second):
        if gathered is None:
            return
        many = -(-len(others.pairs) // (pl.num_programs(0) - 2))
        for number, pair in enumerate(others.pairs):
            when, late = 1 + number // many, number % many >= (many + 1) // 2
            if late == second:

                @pl.when(t == when)
                def _(pair=pair):
                    for piece in pair:
                        piece.start()

                @pl.when(t == when + 1)
                def _(pair=pair):
                    for piece in pair:
                        piece.relay()

    @pl.when(t == 0)
    def _():
        ring.meet()
        if gathered is not None:
            others.start()
        copy = pltpu.make_async_copy(h_hbm, h_ref, local_sem)
        copy.start()
        copy.wait()
        for c in range(CHUNKS):
            part = pl.ds(c * size, size)
            a = normed(h_ref[part])
            a_ref[part] = a
            at_ref[:, part] = a.T
            dyt_ref[:, part] = dy_ref[part].T
            if wanted:
                da_ref[part] = jnp.zeros((size, d), F32)

    def joined(refs, axis):
        return jnp.concatenate([ref[0] for ref in refs], axis)

    def chunk(c):
        wg, wu, wd = joined(wg_refs, 1), joined(wu_refs, 1), joined(wd_refs, 0)
        part = pl.ds(c * size, size)
        a = a_ref[part]
        gate, up = dot(a, wg), dot(a, wu)
        dhid = dot(dy_ref[part], wd, ((1,), (1,))).astype(BF16).astype(F32)
        s = jax.nn.sigmoid(gate)
        silu = gate * s
        hid_ref[part] = (silu * up).astype(BF16)
        dup = (dhid * silu).astype(BF16)
        dgate = (dhid * up * (s * (1 + gate * (1 - s)))).astype(BF16)
        dup_ref[part] = dup
        dgate_ref[part] = dgate
        if wanted:
            da_ref[part] += dot(dgate, wg, ((1,), (1,))) + dot(dup, wu, ((1,), (1,)))

    def put(g, half):
        for place in range(side):
            ga[place, half] = g[side * rows * place : side * rows * (place + 1), :LANES].astype(BF16)
            mine = [g[rows * (side * x + place) : rows * (side * x + place + 1), LANES:] for x in range(side)]
            gb[place, half] = jnp.concatenate(mine, 0).astype(BF16)

    computing, summing = t < steps, t > 0

    @pl.when(computing)
    def _():
        chunk(0)
        chunk(1)

    @pl.when(summing)
    def _():
        for one in (first_a, first_b, first_d):
            one.relay()

    if gathered is not None:

        @pl.when(t == 1)
        def _():
            others.arrive()

    beside(False)

    @pl.when(computing)
    def _():
        chunk(2)
        chunk(3)
        g = dot(dyt_ref[...], hid_ref[...]).T.astype(BF16)
        held_ref[...] = g.reshape(held_ref.shape)

    if gathered is not None:

        @pl.when(t == 0)
        def _():
            others.relay()

    @pl.when(summing)
    def _():
        for one in (first_a, first_b, first_d):
            one.arrive()
        for one, two, total in ((first_a, second_a, sa), (first_b, second_b, sb)):
            place = ring.place(one.axis, 0)
            for half in range(2):
                value = one.terms[place, half].astype(F32) + one.received(half)
                total[half] = value
                for p in range(side):
                    two.terms[p, half] = value[rows * p : rows * (p + 1)].astype(BF16)
                two.first(half).start()
        place = ring.place(0, 0)
        for half in range(2):
            value = gd[place, half].astype(F32) + first_d.received(half)
            count = value.shape[0]
            sd[pl.ds(pl.multiple_of((2 * (t - 1) + half) * count, count), count)] = value

    def mine(place, half):
        return sd[pl.ds(pl.multiple_of((2 * place + half) * half_d, 8), half_d)]

    @pl.when(t == steps)
    def _():
        for p in range(side):
            for half in range(2):
                hd[p, half] = mine(p, half).astype(BF16)
        for half in range(2):
            second_d.first(half).start()

    @pl.when(computing)
    def _():
        gd[...] = held_ref[...]
        for half in range(2):
            first_d.first(half).start()
        g = dot(at_ref[...], dgate_ref[...])
        put(g, 0)
        first_a.first(0).start()
        first_b.first(0).start()

    def own(total):
        return lambda place, half: total[half, pl.ds(pl.multiple_of(place * rows, 8), rows)]

    @pl.when(summing)
    def _():
        second_a.relay(own(sa))
        second_b.relay(own(sb))

    @pl.when(t == steps)
    def _():
        second_d.relay(mine)

    beside(True)

    @pl.when(computing)
    def _():
        g = dot(at_ref[...], dup_ref[...])
        put(g, 1)
        first_a.first(1).start()
        first_b.first(1).start()

    @pl.when(summing)
    def _():
        second_a.arrive()
        second_b.arrive()
        for two, total, tile in ((second_a, sa, 0), (second_b, sb, 1)):
            place = ring.place(two.axis, 0)
            for half, out in enumerate((gg_ref, gu_ref)):
                value = (own(total)(place, half) + two.received(half)).astype(BF16)
                for j in range(value.shape[1] // LANES):
                    lane = pl.multiple_of((t - 1 + steps * (tile + j)) * LANES, LANES)
                    out[:, pl.ds(lane, LANES)] = value[:, j * LANES : (j + 1) * LANES]

    if wanted:

        @pl.when(t == steps - 1)
        def _():
            for c in range(CHUNKS):
                part = pl.ds(c * size, size)
                wide = h_ref[part].astype(F32)
                by_a = da_ref[part].astype(BF16).astype(F32)
                scale = lax.rsqrt(jnp.mean(wide**2, -1, keepdims=True) + 1e-6)
                along = jnp.mean(by_a * wide, -1, keepdims=True)
                by_h = by_a * scale - wide * (along * scale * scale * scale)
                h_ref[part] = dy_ref[part] + by_h.astype(BF16)

    @pl.when(t == steps)
    def _():
        second_d.arrive()
        place = ring.place(1, 0)
        for half in range(2):
            gd_ref[half * half_d : (half + 1) * half_d] = (mine(place, half) + second_d.received(half)).astype(BF16)
        if gathered is not None:
            others.finish()


def backward(side, h, dy, wg, wu, wd, layer, wanted, shards=(), gathered=None):
    tokens, d = h.shape
    ff = wg.shape[2]
    tiles = ff // LANES
    steps = tiles // side
    rows, down_rows = d // side**2, ff // side**2
    width = side * LANES

    def tile(j):
        return lambda t: jnp.minimum(t, steps - 1) + steps * j

    across = [pl.BlockSpec((1, d, LANES), lambda t, j=j: (layer, 0, tile(j)(t))) for j in range(side)]
    down = [pl.BlockSpec((1, LANES, d), lambda t, j=j: (layer, tile(j)(t), 0)) for j in range(side)]
    shapes = [(side, 2, side * rows, LANES), (side, 2, side * rows, width - LANES), (side, 2, LANES // 2, d)]
    shapes2 = [(side, 2, rows, LANES), (side, 2, rows, width - LANES), (side, 2, down_rows // 2, d)]

    def buffers(shapes):
        terms = [pltpu.VMEM(s, BF16) for s in shapes]
        far = [pltpu.VMEM(s[1:], BF16) for s in shapes]
        near = [pltpu.VMEM((2, *s[1:]), BF16) for s in shapes]
        return terms + far + near

    totals = [
        pltpu.VMEM((2, side * rows, LANES), F32),
        pltpu.VMEM((2, side * rows, width - LANES), F32),
        pltpu.VMEM((side * down_rows, d), F32),
    ]
    scratch = [
        pltpu.VMEM((tokens, d), BF16),
        pltpu.VMEM((d, tokens), BF16),
        pltpu.VMEM((d, tokens), BF16),
        pltpu.VMEM((tokens, width), BF16),
        pltpu.VMEM((tokens, width), BF16),
        pltpu.VMEM((tokens, width), BF16),
        pltpu.VMEM(shapes[2], BF16),
        pltpu.SemaphoreType.DMA,
        *buffers(shapes),
        *totals,
        *buffers(shapes2),
        pltpu.SemaphoreType.DMA((6, 2, 4)),
    ]
    results = [(rows, ff), (rows, ff), (down_rows, d)] + [(tokens, d)] * wanted
    out_specs = [whole(s) for s in results]
    out_shape = [jax.ShapeDtypeStruct(s, BF16) for s in results]
    scratch.append(pltpu.VMEM((tokens, d), F32 if wanted else BF16))
    if shards:
        out_specs += [pl.BlockSpec(memory_space=pl.ANY)] * 3
        out_shape += [jax.ShapeDtypeStruct(w.shape, w.dtype) for w in (wg, wu, wd)]
        scratch += gather_scratch(side)
    return pl.pallas_call(
        functools.partial(backward_kernel, side, wanted, gathered),
        grid=(steps + 1,),
        in_specs=[pl.BlockSpec(memory_space=pl.ANY), whole((tokens, d)), *across, *across, *down, *(whole(s.shape) for s in shards)],
        out_specs=out_specs,
        out_shape=out_shape,
        scratch_shapes=scratch,
        cost_estimate=pl.CostEstimate(
            flops=2 * tokens * d * ff * (8 if wanted else 6), bytes_accessed=6 * 2 * d * ff, transcendentals=tokens * ff
        ),
        compiler_params=pltpu.CompilerParams(vmem_limit_bytes=63 * 2**20, collective_id=1 + layer, has_side_effects=True),
        name=f"backward_{layer}",
    )(h, dy, *[wg] * side, *[wu] * side, *[wd] * side, *shards)


def gather_kernel(side, layer, *refs):
    shards, outs, (sems, local_sems) = refs[:3], refs[6:9], refs[9:]
    ring = Ring(side)
    ring.meet()
    all_of = Gather(ring, shards, outs, layer, sems, local_sems)
    all_of.start()
    all_of.relay()
    all_of.arrive()
    for pair in all_of.pairs:
        for piece in pair:
            piece.start()
    for pair in all_of.pairs:
        for piece in pair:
            piece.relay()
    all_of.finish()


def gather_scratch(side):
    return [pltpu.SemaphoreType.DMA((2, 6 * (1 + side), 4)), pltpu.SemaphoreType.DMA((3,))]


def gather(side, layer, shards, weights):
    hbm = pl.BlockSpec(memory_space=pl.ANY)
    return pl.pallas_call(
        functools.partial(gather_kernel, side, layer),
        in_specs=[pl.BlockSpec(memory_space=pltpu.VMEM)] * 3 + [hbm] * 3,
        out_specs=[hbm] * 3,
        out_shape=[jax.ShapeDtypeStruct(w.shape, w.dtype) for w in weights],
        input_output_aliases={3: 0, 4: 1, 5: 2},
        scratch_shapes=gather_scratch(side),
        compiler_params=pltpu.CompilerParams(vmem_limit_bytes=60 * 2**20, collective_id=0, has_side_effects=True),
        name="gather",
    )(*shards, *weights)


def solution(mesh):
    side = math.isqrt(mesh.shape["dp"])

    def step(x, dy, *arrays):
        weights, ms, vs = (arrays[i : i + 3] for i in (0, 3, 6))
        x, dy = x[0], dy[0]
        layers = weights[0].shape[0]
        me = lax.axis_index("dp")

        states = [x]
        for n in range(layers - 1):
            states.append(forward(states[-1], *weights, n))

        def of_mine(which):
            w, rows = weights[which], ms[which].shape[1]
            return lax.dynamic_slice_in_dim(w, me * rows, rows, 1).astype(F32)

        def fresh(n):
            return [adamw(of_mine(i)[n], ms[i][n], vs[i][n], grads[n][i].astype(F32))[0] for i in range(3)]

        grads, shards = [None] * layers, ()
        for n in reversed(range(layers)):
            *out, = backward(side, states[n], dy, *weights, n, n > 0, shards, n + 1 if shards else None)
            grads[n], gathered = out[:3], out[-3:]
            dy = out[3]
            shards = fresh(n)
        gathered = gather(side, 0, shards, gathered)
        moments = []
        for i in range(3):
            g = jnp.stack([grads[n][i] for n in range(layers)]).astype(F32)
            moments.append(adamw(of_mine(i), ms[i], vs[i], g)[1:])
        return (*gathered, *(one[0] for one in moments), *(one[1] for one in moments))

    tokens, row = P(("rep", "dp"), None, None), P(None, "dp", None)
    return jax.shard_map(
        step,
        mesh=mesh,
        in_specs=(tokens,) * 2 + (P(),) * 3 + (row,) * 6,
        out_specs=(P("rep", None, None),) * 3 + (P("rep", "dp", None),) * 6,
        check_vma=False,
    )
```

```python
import functools
import math

import jax
import jax.numpy as jnp
from jax import lax
from jax.experimental import pallas as pl
from jax.experimental.pallas import tpu as pltpu
from jax.sharding import PartitionSpec as P

BLOCK = 256
CHUNKS = 4
LANES = 128
MESH = pl.DeviceIdType.MESH
F32, BF16 = jnp.float32, jnp.bfloat16


def dot(a, b, contract=((1,), (0,))):
    return lax.dot_general(a, b, (contract, ((), ())), preferred_element_type=F32)


def normed(h):
    wide = h.astype(F32)
    scale = lax.rsqrt(jnp.mean(wide**2, -1, keepdims=True) + 1e-6)
    return (wide * scale).astype(BF16)


def moments(m, v, g):
    return 0.9 * m + 0.1 * g, 0.95 * v + 0.05 * g * g


def adamw(w, m, v, g):
    m, v = moments(m, v, g)
    step = m * lax.rsqrt(v + 1e-8) + 0.1 * w
    return (w - 0.02 * step).astype(BF16)


def whole(shape):
    return pl.BlockSpec(shape, lambda *_: (0,) * len(shape), pipeline_mode=pl.Buffered(1))


def forward_kernel(x_ref, wg_ref, wu_ref, wd_ref, h_ref, a_ref, acc_ref):
    tokens = x_ref.shape[0]
    chunks, CHUNK = CHUNKS, tokens // CHUNKS
    f = pl.program_id(0)

    @pl.when(f == 0)
    def _():
        @pl.loop(0, chunks)
        def _(c):
            rows = pl.ds(c * CHUNK, CHUNK)
            a_ref[rows] = normed(x_ref[rows])
            acc_ref[rows] = jnp.zeros((CHUNK, x_ref.shape[1]), F32)

    wg, wu, wd = wg_ref[0], wu_ref[0], wd_ref[0]
    for c in range(chunks):
        rows = pl.ds(c * CHUNK, CHUNK)
        a = a_ref[rows]
        gate, up = dot(a, wg), dot(a, wu)
        hidden = (gate * jax.nn.sigmoid(gate) * up).astype(BF16)
        acc_ref[rows] += dot(hidden, wd)

    @pl.when(f == pl.num_programs(0) - 1)
    def _():
        @pl.loop(0, chunks)
        def _(c):
            rows = pl.ds(c * CHUNK, CHUNK)
            h_ref[rows] = x_ref[rows] + acc_ref[rows].astype(BF16)


def forward(x, wg, wu, wd, layer):
    tokens, d = x.shape
    ff = wg.shape[2]
    cost = 6 * tokens * d * ff
    return pl.pallas_call(
        forward_kernel,
        grid=(ff // BLOCK,),
        in_specs=[
            whole((tokens, d)),
            pl.BlockSpec((1, d, BLOCK), lambda f: (layer, 0, f)),
            pl.BlockSpec((1, d, BLOCK), lambda f: (layer, 0, f)),
            pl.BlockSpec((1, BLOCK, d), lambda f: (layer, f, 0)),
        ],
        out_specs=whole((tokens, d)),
        out_shape=jax.ShapeDtypeStruct((tokens, d), BF16),
        scratch_shapes=[pltpu.VMEM((tokens, d), BF16), pltpu.VMEM((tokens, d), F32)],
        cost_estimate=pl.CostEstimate(flops=cost, bytes_accessed=3 * 2 * d * ff, transcendentals=tokens * ff),
        compiler_params=pltpu.CompilerParams(vmem_limit_bytes=60 * 2**20),
        name="forward",
    )(x, wg, wu, wd)


class Ring:
    def __init__(self, side):
        me = lax.axis_index("dp")
        self.side = side
        self.at = (lax.div(me, side), lax.rem(me, side))

    def place(self, axis, offset):
        return lax.rem(self.at[axis] + offset + self.side, self.side)

    def device(self, axis, offset):
        there = [self.at[0], self.at[1]]
        there[axis] = self.place(axis, offset)
        return {"dp": there[0] * self.side + there[1]}

    def meet(self):
        barrier = pltpu.get_barrier_semaphore()
        for axis in range(2):
            for offset in (1, -1):
                pl.semaphore_signal(barrier, inc=1, device_id=self.device(axis, offset), device_id_type=MESH)
        pl.semaphore_wait(barrier, 4)


class Scatter:
    def __init__(self, ring, axis, terms, far, near, sems):
        self.ring, self.axis, self.terms, self.far, self.near, self.sems = ring, axis, terms, far, near, sems

    def copy(self, src, dst, number, offset):
        return pltpu.make_async_remote_copy(
            src_ref=src,
            dst_ref=dst,
            send_sem=self.sems.at[0, number],
            recv_sem=self.sems.at[1, number],
            device_id=self.ring.device(self.axis, offset),
            device_id_type=MESH,
        )

    def first(self, half):
        opposite = self.ring.place(self.axis, 2)
        return self.copy(self.terms.at[opposite, half], self.far.at[half], half, 1 - 2 * half)

    def second(self, side):
        offset = 1 - 2 * side
        return self.copy(self.terms.at[self.ring.place(self.axis, offset)], self.near.at[side], 2 + side, offset)

    def relay(self, own=None):
        for side in range(2):
            self.first(side).wait()
            place = self.ring.place(self.axis, 1 - 2 * side)
            term = self.terms[place, side].astype(F32) if own is None else own(place, side)
            self.terms[place, side] = (term + self.far[side].astype(F32)).astype(BF16)
        for side in range(2):
            self.second(side).start()

    def arrive(self):
        for side in range(2):
            self.second(side).wait()

    def received(self, half):
        return self.near[0, half].astype(F32) + self.near[1, half].astype(F32)


class Piece:
    def __init__(self, ring, axis, src, block, part, sems, number):
        self.ring, self.axis, self.src, self.block, self.part, self.sems, self.number = ring, axis, src, block, part, sems, number

    def copy(self, src, dst, which, offset):
        return pltpu.make_async_remote_copy(
            src_ref=src,
            dst_ref=dst,
            send_sem=self.sems.at[0, self.number, which],
            recv_sem=self.sems.at[1, self.number, which],
            device_id=self.ring.device(self.axis, offset),
            device_id_type=MESH,
        )

    def near(self, side):
        return self.copy(self.block(0) if self.src is None else self.src, self.block(0), side, 1 - 2 * side)

    def far(self, side):
        offset = 1 - 2 * side
        return self.copy(self.part(-offset, side), self.part(-offset, side), 2 + side, offset)

    def start(self):
        for side in range(2):
            self.near(side).start()

    def relay(self):
        for side in range(2):
            self.near(side).wait_recv()
            self.far(side).start()

    def arrive(self):
        for side in range(2):
            self.far(side).wait_recv()

    def sent(self):
        for side in range(2):
            self.near(side).wait_send()
            self.far(side).wait_send()


class Gather:
    def __init__(self, ring, shards, outs, layer, sems, local_sems):
        self.ring, self.shards, self.outs, self.layer, self.local_sems = ring, shards, outs, layer, local_sems
        side = ring.side
        self.ones, self.pairs = [], []
        for i in range(3):
            pair = [[] for _ in range(side)]
            for half in range(2):
                axis = 1 - half
                unit = 2 * i + half

                def owner(offset, axis=axis):
                    at = [ring.at[0], ring.at[1]]
                    at[axis] = ring.place(axis, offset)
                    return at[0] * side + at[1]

                self.ones.append(self.piece(i, half, axis, owner, self.region(shards[i], i, 0, half), sems, unit))
                for k in range(side):

                    def owner(offset, axis=axis, k=k):
                        at = [k, k]
                        at[1 - axis] = ring.place(1 - axis, offset)
                        return at[0] * side + at[1]

                    pair[k].append(self.piece(i, half, 1 - axis, owner, None, sems, 6 + unit * side + k))
            self.pairs += pair

    def piece(self, i, half, axis, owner, src, sems, number):
        out = self.outs[i].at[self.layer]
        return Piece(
            self.ring,
            axis,
            src,
            lambda offset: self.region(out, i, owner(offset), half),
            lambda offset, part: self.region(out, i, owner(offset), half, part),
            sems,
            number,
        )

    def region(self, ref, i, owner, half, part=None):
        rows, columns = self.shards[i].shape
        share = 2 if part is None else 4
        which = half if part is None else 2 * half + part
        if columns % (4 * LANES) == 0:
            first = owner * rows
            return ref.at[pl.ds(pl.multiple_of(first, 8), rows), pl.ds(which * (columns // share), columns // share)]
        length = rows // share
        return ref.at[pl.ds(pl.multiple_of(owner * rows + which * length, 8), length)]

    def local(self, i):
        rows = self.shards[i].shape[0]
        me = self.ring.at[0] * self.ring.side + self.ring.at[1]
        out = self.outs[i].at[self.layer, pl.ds(pl.multiple_of(me * rows, 8), rows)]
        return pltpu.make_async_copy(self.shards[i], out, self.local_sems.at[i])

    def start(self):
        for one in self.ones:
            one.start()
        for i in range(3):
            self.local(i).start()

    def relay(self):
        for one in self.ones:
            one.relay()

    def arrive(self):
        for one in self.ones:
            one.arrive()
        for i in range(3):
            self.local(i).wait()

    def finish(self):
        for pair in self.pairs:
            for piece in pair:
                piece.arrive()
        for one in (*self.ones, *(piece for pair in self.pairs for piece in pair)):
            one.sent()


def backward_kernel(side, wanted, gathered, h_hbm, dy_ref, *refs):
    wg_refs, wu_refs, wd_refs, refs = refs[:side], refs[side : 2 * side], refs[2 * side : 3 * side], refs[3 * side :]
    if gathered is not None:
        shards, refs = refs[:3], refs[3:]
    gg_ref, gu_ref, gd_ref, *refs = refs
    if wanted:
        h_ref, *refs = refs
    if gathered is not None:
        outs, refs = refs[:3], refs[3:]
    a_ref, at_ref, dyt_ref, hid_ref, dgate_ref, dup_ref, held_ref, local_sem, refs = *refs[:8], refs[8:]
    ga, gb, gd, ra, rb, rd, na, nb, nd, sa, sb, sd, refs = *refs[:12], refs[12:]
    ha, hb, hd, ra2, rb2, rd2, na2, nb2, nd2, sems, refs = *refs[:10], refs[10:]
    if wanted:
        da_ref, *refs = refs
    else:
        h_ref, *refs = refs
    tokens, d = dy_ref.shape
    size = tokens // CHUNKS
    t, steps = pl.program_id(0), pl.num_programs(0) - 1
    rows = gg_ref.shape[0]
    ring = Ring(side)
    half_d = hd.shape[2]
    first_a, first_b, first_d = (
        Scatter(ring, axis, g, r, n, sems.at[i]) for i, (axis, g, r, n) in enumerate(((0, ga, ra, na), (1, gb, rb, nb), (0, gd, rd, nd)))
    )
    second_a, second_b, second_d = (
        Scatter(ring, axis, g, r, n, sems.at[3 + i])
        for i, (axis, g, r, n) in enumerate(((1, ha, ra2, na2), (0, hb, rb2, nb2), (1, hd, rd2, nd2)))
    )

    if gathered is not None:
        others = Gather(ring, shards, outs, gathered, *refs)

    def beside(second):
        if gathered is None:
            return
        many = -(-len(others.pairs) // (pl.num_programs(0) - 2))
        for number, pair in enumerate(others.pairs):
            when, late = 1 + number // many, number % many >= (many + 1) // 2
            if late == second:

                @pl.when(t == when)
                def _(pair=pair):
                    for piece in pair:
                        piece.start()

                @pl.when(t == when + 1)
                def _(pair=pair):
                    for piece in pair:
                        piece.relay()

    @pl.when(t == 0)
    def _():
        ring.meet()
        if gathered is not None:
            others.start()
        copy = pltpu.make_async_copy(h_hbm, h_ref, local_sem)
        copy.start()
        copy.wait()
        for c in range(CHUNKS):
            part = pl.ds(c * size, size)
            a = normed(h_ref[part])
            a_ref[part] = a
            at_ref[:, part] = a.T
            dyt_ref[:, part] = dy_ref[part].T
            if wanted:
                da_ref[part] = jnp.zeros((size, d), F32)

    def joined(refs, axis):
        return jnp.concatenate([ref[0] for ref in refs], axis)

    def chunk(c):
        wg, wu, wd = joined(wg_refs, 1), joined(wu_refs, 1), joined(wd_refs, 0)
        part = pl.ds(c * size, size)
        a = a_ref[part]
        gate, up = dot(a, wg), dot(a, wu)
        dhid = dot(dy_ref[part], wd, ((1,), (1,))).astype(BF16).astype(F32)
        s = jax.nn.sigmoid(gate)
        silu = gate * s
        hid_ref[part] = (silu * up).astype(BF16)
        dup = (dhid * silu).astype(BF16)
        dgate = (dhid * up * (s * (1 + gate * (1 - s)))).astype(BF16)
        dup_ref[part] = dup
        dgate_ref[part] = dgate
        if wanted:
            da_ref[part] += dot(dgate, wg, ((1,), (1,))) + dot(dup, wu, ((1,), (1,)))

    def put(g, half):
        for place in range(side):
            ga[place, half] = g[side * rows * place : side * rows * (place + 1), :LANES].astype(BF16)
            mine = [g[rows * (side * x + place) : rows * (side * x + place + 1), LANES:] for x in range(side)]
            gb[place, half] = jnp.concatenate(mine, 0).astype(BF16)

    def own(total):
        return lambda place, half: total[half, pl.ds(pl.multiple_of(place * rows, 8), rows)]

    def mine(place, half):
        return sd[pl.ds(pl.multiple_of((2 * place + half) * half_d, 8), half_d)]

    def second_relay():
        second_a.relay(own(sa))
        second_b.relay(own(sb))

    def second_end(run):
        second_a.arrive()
        second_b.arrive()
        for two, total, tile in ((second_a, sa, 0), (second_b, sb, 1)):
            place = ring.place(two.axis, 0)
            for half, out in enumerate((gg_ref, gu_ref)):
                value = (own(total)(place, half) + two.received(half)).astype(BF16)
                for j in range(value.shape[1] // LANES):
                    lane = pl.multiple_of((run + steps * (tile + j)) * LANES, LANES)
                    out[:, pl.ds(lane, LANES)] = value[:, j * LANES : (j + 1) * LANES]

    computing, summing, ending = t < steps, t > 0, t > 1

    @pl.when(computing)
    def _():
        chunk(0)
        chunk(1)

    @pl.when(ending)
    def _():
        second_relay()

    @pl.when(summing)
    def _():
        for one in (first_a, first_b, first_d):
            one.relay()

    if gathered is not None:

        @pl.when(t == 1)
        def _():
            others.arrive()

    beside(False)

    @pl.when(computing)
    def _():
        chunk(2)
        chunk(3)
        g = dot(dyt_ref[...], hid_ref[...]).T.astype(BF16)
        held_ref[...] = g.reshape(held_ref.shape)

    if gathered is not None:

        @pl.when(t == 0)
        def _():
            others.relay()

    @pl.when(ending)
    def _():
        second_end(t - 2)

    @pl.when(summing)
    def _():
        for one in (first_a, first_b, first_d):
            one.arrive()
        for one, two, total in ((first_a, second_a, sa), (first_b, second_b, sb)):
            place = ring.place(one.axis, 0)
            for half in range(2):
                value = one.terms[place, half].astype(F32) + one.received(half)
                total[half] = value
                for p in range(side):
                    two.terms[p, half] = value[rows * p : rows * (p + 1)].astype(BF16)
                two.first(half).start()
        place = ring.place(0, 0)
        for half in range(2):
            value = gd[place, half].astype(F32) + first_d.received(half)
            count = value.shape[0]
            sd[pl.ds(pl.multiple_of((2 * (t - 1) + half) * count, count), count)] = value

    @pl.when(t == steps)
    def _():
        for p in range(side):
            for half in range(2):
                hd[p, half] = mine(p, half).astype(BF16)
        for half in range(2):
            second_d.first(half).start()

    @pl.when(computing)
    def _():
        gd[...] = held_ref[...]
        for half in range(2):
            first_d.first(half).start()

    beside(True)

    @pl.when(computing)
    def _():
        g = dot(at_ref[...], dgate_ref[...])
        put(g, 0)
        first_a.first(0).start()
        first_b.first(0).start()

    @pl.when(computing)
    def _():
        g = dot(at_ref[...], dup_ref[...])
        put(g, 1)
        first_a.first(1).start()
        first_b.first(1).start()

    if wanted:

        @pl.when(t == steps - 1)
        def _():
            for c in range(CHUNKS):
                part = pl.ds(c * size, size)
                wide = h_ref[part].astype(F32)
                by_a = da_ref[part].astype(BF16).astype(F32)
                scale = lax.rsqrt(jnp.mean(wide**2, -1, keepdims=True) + 1e-6)
                along = jnp.mean(by_a * wide, -1, keepdims=True)
                by_h = by_a * scale - wide * (along * scale * scale * scale)
                h_ref[part] = dy_ref[part] + by_h.astype(BF16)

    @pl.when(t == steps)
    def _():
        second_relay()
        second_d.relay(mine)
        second_end(t - 1)
        second_d.arrive()
        place = ring.place(1, 0)
        for half in range(2):
            gd_ref[half * half_d : (half + 1) * half_d] = (mine(place, half) + second_d.received(half)).astype(BF16)
        if gathered is not None:
            others.finish()


def backward(side, h, dy, wg, wu, wd, layer, wanted, shards=(), gathered=None):
    tokens, d = h.shape
    ff = wg.shape[2]
    tiles = ff // LANES
    steps = tiles // side
    rows, down_rows = d // side**2, ff // side**2
    width = side * LANES

    def tile(j):
        return lambda t: jnp.minimum(t, steps - 1) + steps * j

    across = [pl.BlockSpec((1, d, LANES), lambda t, j=j: (layer, 0, tile(j)(t))) for j in range(side)]
    down = [pl.BlockSpec((1, LANES, d), lambda t, j=j: (layer, tile(j)(t), 0)) for j in range(side)]
    shapes = [(side, 2, side * rows, LANES), (side, 2, side * rows, width - LANES), (side, 2, LANES // 2, d)]
    shapes2 = [(side, 2, rows, LANES), (side, 2, rows, width - LANES), (side, 2, down_rows // 2, d)]

    def buffers(shapes):
        terms = [pltpu.VMEM(s, BF16) for s in shapes]
        far = [pltpu.VMEM(s[1:], BF16) for s in shapes]
        near = [pltpu.VMEM((2, *s[1:]), BF16) for s in shapes]
        return terms + far + near

    totals = [
        pltpu.VMEM((2, side * rows, LANES), F32),
        pltpu.VMEM((2, side * rows, width - LANES), F32),
        pltpu.VMEM((side * down_rows, d), F32),
    ]
    scratch = [
        pltpu.VMEM((tokens, d), BF16),
        pltpu.VMEM((d, tokens), BF16),
        pltpu.VMEM((d, tokens), BF16),
        pltpu.VMEM((tokens, width), BF16),
        pltpu.VMEM((tokens, width), BF16),
        pltpu.VMEM((tokens, width), BF16),
        pltpu.VMEM(shapes[2], BF16),
        pltpu.SemaphoreType.DMA,
        *buffers(shapes),
        *totals,
        *buffers(shapes2),
        pltpu.SemaphoreType.DMA((6, 2, 4)),
    ]
    results = [(rows, ff), (rows, ff), (down_rows, d)] + [(tokens, d)] * wanted
    out_specs = [whole(s) for s in results]
    out_shape = [jax.ShapeDtypeStruct(s, BF16) for s in results]
    scratch.append(pltpu.VMEM((tokens, d), F32 if wanted else BF16))
    if shards:
        out_specs += [pl.BlockSpec(memory_space=pl.ANY)] * 3
        out_shape += [jax.ShapeDtypeStruct(w.shape, w.dtype) for w in (wg, wu, wd)]
        scratch += gather_scratch(side)
    return pl.pallas_call(
        functools.partial(backward_kernel, side, wanted, gathered),
        grid=(steps + 1,),
        in_specs=[pl.BlockSpec(memory_space=pl.ANY), whole((tokens, d)), *across, *across, *down, *(whole(s.shape) for s in shards)],
        out_specs=out_specs,
        out_shape=out_shape,
        scratch_shapes=scratch,
        cost_estimate=pl.CostEstimate(
            flops=2 * tokens * d * ff * (8 if wanted else 6), bytes_accessed=6 * 2 * d * ff, transcendentals=tokens * ff
        ),
        compiler_params=pltpu.CompilerParams(vmem_limit_bytes=63 * 2**20, collective_id=1 + layer, has_side_effects=True),
        name=f"backward_{layer}",
    )(h, dy, *[wg] * side, *[wu] * side, *[wd] * side, *shards)


def gather_kernel(side, layer, *refs):
    shards, outs, (sems, local_sems) = refs[:3], refs[6:9], refs[9:]
    ring = Ring(side)
    ring.meet()
    all_of = Gather(ring, shards, outs, layer, sems, local_sems)
    all_of.start()
    all_of.relay()
    all_of.arrive()
    for pair in all_of.pairs:
        for piece in pair:
            piece.start()
    for pair in all_of.pairs:
        for piece in pair:
            piece.relay()
    all_of.finish()


def gather_scratch(side):
    return [pltpu.SemaphoreType.DMA((2, 6 * (1 + side), 4)), pltpu.SemaphoreType.DMA((3,))]


def gather(side, layer, shards, weights):
    hbm = pl.BlockSpec(memory_space=pl.ANY)
    return pl.pallas_call(
        functools.partial(gather_kernel, side, layer),
        in_specs=[pl.BlockSpec(memory_space=pltpu.VMEM)] * 3 + [hbm] * 3,
        out_specs=[hbm] * 3,
        out_shape=[jax.ShapeDtypeStruct(w.shape, w.dtype) for w in weights],
        input_output_aliases={3: 0, 4: 1, 5: 2},
        scratch_shapes=gather_scratch(side),
        compiler_params=pltpu.CompilerParams(vmem_limit_bytes=60 * 2**20, collective_id=0, has_side_effects=True),
        name="gather",
    )(*shards, *weights)


def solution(mesh):
    side = math.isqrt(mesh.shape["dp"])

    def step(x, dy, *arrays):
        weights, ms, vs = (arrays[i : i + 3] for i in (0, 3, 6))
        x, dy = x[0], dy[0]
        layers = weights[0].shape[0]
        me = lax.axis_index("dp")

        states = [x]
        for n in range(layers - 1):
            states.append(forward(states[-1], *weights, n))

        def fresh(n):
            new = []
            for i in range(3):
                rows, columns = ms[i].shape[1:]
                w = lax.dynamic_slice(weights[i], (n, me * rows, 0), (1, rows, columns))[0]
                new.append(adamw(w.astype(F32), ms[i][n], vs[i][n], grads[n][i].astype(F32)))
            return new

        grads, shards = [None] * layers, ()
        for n in reversed(range(layers)):
            *out, = backward(side, states[n], dy, *weights, n, n > 0, shards, n + 1 if shards else None)
            grads[n], gathered = out[:3], out[-3:]
            dy = out[3]
            shards = fresh(n)
        gathered = gather(side, 0, shards, gathered)
        after = []
        for i in range(3):
            g = jnp.stack([grads[n][i] for n in range(layers)]).astype(F32)
            after.append(moments(ms[i], vs[i], g))
        return (*gathered, *(one[0] for one in after), *(one[1] for one in after))

    tokens, row = P(("rep", "dp"), None, None), P(None, "dp", None)
    return jax.shard_map(
        step,
        mesh=mesh,
        in_specs=(tokens,) * 2 + (P(),) * 3 + (row,) * 6,
        out_specs=(P("rep", None, None),) * 3 + (P("rep", "dp", None),) * 6,
        check_vma=False,
    )
```

```python
import functools
import math

import jax
import jax.numpy as jnp
from jax import lax
from jax.experimental import pallas as pl
from jax.experimental.pallas import tpu as pltpu
from jax.sharding import PartitionSpec as P

BLOCK = 512
CHUNKS = 4
LANES = 128
MESH = pl.DeviceIdType.MESH
F32, BF16 = jnp.float32, jnp.bfloat16


def dot(a, b, contract=((1,), (0,))):
    return lax.dot_general(a, b, (contract, ((), ())), preferred_element_type=F32)


def normed(h):
    wide = h.astype(F32)
    scale = lax.rsqrt(jnp.mean(wide**2, -1, keepdims=True) + 1e-6)
    return (wide * scale).astype(BF16)


def moments(m, v, g):
    return 0.9 * m + 0.1 * g, 0.95 * v + 0.05 * g * g


def adamw(w, m, v, g):
    m, v = moments(m, v, g)
    step = m * lax.rsqrt(v + 1e-8) + 0.1 * w
    return (w - 0.02 * step).astype(BF16)


def whole(shape):
    return pl.BlockSpec(shape, lambda *_: (0,) * len(shape), pipeline_mode=pl.Buffered(1))


def forward_kernel(x_ref, wg_ref, wu_ref, wd_ref, h_ref, a_ref, acc_ref):
    tokens = x_ref.shape[0]
    chunks, CHUNK = CHUNKS, tokens // CHUNKS
    f = pl.program_id(0)

    @pl.when(f == 0)
    def _():
        @pl.loop(0, chunks)
        def _(c):
            rows = pl.ds(c * CHUNK, CHUNK)
            a_ref[rows] = normed(x_ref[rows])
            acc_ref[rows] = jnp.zeros((CHUNK, x_ref.shape[1]), F32)

    wg, wu, wd = wg_ref[0], wu_ref[0], wd_ref[0]
    @pl.loop(0, chunks // 2)
    def _(i):
        for c in range(2):
            rows = pl.ds((2 * i + c) * CHUNK, CHUNK)
            a = a_ref[rows]
            gate, up = dot(a, wg), dot(a, wu)
            hidden = (gate * jax.nn.sigmoid(gate) * up).astype(BF16)
            acc_ref[rows] += dot(hidden, wd)

    @pl.when(f == pl.num_programs(0) - 1)
    def _():
        @pl.loop(0, chunks)
        def _(c):
            rows = pl.ds(c * CHUNK, CHUNK)
            h_ref[rows] = x_ref[rows] + acc_ref[rows].astype(BF16)


def forward(x, wg, wu, wd, layer):
    tokens, d = x.shape
    ff = wg.shape[2]
    cost = 6 * tokens * d * ff
    return pl.pallas_call(
        forward_kernel,
        grid=(ff // BLOCK,),
        in_specs=[
            whole((tokens, d)),
            pl.BlockSpec((1, d, BLOCK), lambda f: (layer, 0, f)),
            pl.BlockSpec((1, d, BLOCK), lambda f: (layer, 0, f)),
            pl.BlockSpec((1, BLOCK, d), lambda f: (layer, f, 0)),
        ],
        out_specs=whole((tokens, d)),
        out_shape=jax.ShapeDtypeStruct((tokens, d), BF16),
        scratch_shapes=[pltpu.VMEM((tokens, d), BF16), pltpu.VMEM((tokens, d), F32)],
        cost_estimate=pl.CostEstimate(flops=cost, bytes_accessed=3 * 2 * d * ff, transcendentals=tokens * ff),
        compiler_params=pltpu.CompilerParams(vmem_limit_bytes=60 * 2**20),
        name="forward",
    )(x, wg, wu, wd)


class Ring:
    def __init__(self, side):
        me = lax.axis_index("dp")
        self.side = side
        self.at = (lax.div(me, side), lax.rem(me, side))

    def place(self, axis, offset):
        return lax.rem(self.at[axis] + offset + self.side, self.side)

    def device(self, axis, offset):
        there = [self.at[0], self.at[1]]
        there[axis] = self.place(axis, offset)
        return {"dp": there[0] * self.side + there[1]}

    def meet(self):
        barrier = pltpu.get_barrier_semaphore()
        for axis in range(2):
            for offset in (1, -1):
                pl.semaphore_signal(barrier, inc=1, device_id=self.device(axis, offset), device_id_type=MESH)
        pl.semaphore_wait(barrier, 4)


class Scatter:
    def __init__(self, ring, axis, terms, far, near, sems):
        self.ring, self.axis, self.terms, self.far, self.near, self.sems = ring, axis, terms, far, near, sems

    def copy(self, src, dst, number, offset):
        return pltpu.make_async_remote_copy(
            src_ref=src,
            dst_ref=dst,
            send_sem=self.sems.at[0, number],
            recv_sem=self.sems.at[1, number],
            device_id=self.ring.device(self.axis, offset),
            device_id_type=MESH,
        )

    def first(self, half):
        opposite = self.ring.place(self.axis, 2)
        return self.copy(self.terms.at[opposite, half], self.far.at[half], half, 1 - 2 * half)

    def second(self, side):
        offset = 1 - 2 * side
        return self.copy(self.terms.at[self.ring.place(self.axis, offset)], self.near.at[side], 2 + side, offset)

    def relay(self, own=None):
        for side in range(2):
            self.first(side).wait()
            place = self.ring.place(self.axis, 1 - 2 * side)
            term = self.terms[place, side].astype(F32) if own is None else own(place, side)
            self.terms[place, side] = (term + self.far[side].astype(F32)).astype(BF16)
        for side in range(2):
            self.second(side).start()

    def arrive(self):
        for side in range(2):
            self.second(side).wait()

    def received(self, half):
        return self.near[0, half].astype(F32) + self.near[1, half].astype(F32)


class Piece:
    def __init__(self, ring, axis, src, block, part, sems, number):
        self.ring, self.axis, self.src, self.block, self.part, self.sems, self.number = ring, axis, src, block, part, sems, number

    def copy(self, src, dst, which, offset):
        return pltpu.make_async_remote_copy(
            src_ref=src,
            dst_ref=dst,
            send_sem=self.sems.at[0, self.number, which],
            recv_sem=self.sems.at[1, self.number, which],
            device_id=self.ring.device(self.axis, offset),
            device_id_type=MESH,
        )

    def near(self, side):
        return self.copy(self.block(0) if self.src is None else self.src, self.block(0), side, 1 - 2 * side)

    def far(self, side):
        offset = 1 - 2 * side
        return self.copy(self.part(-offset, side), self.part(-offset, side), 2 + side, offset)

    def start(self):
        for side in range(2):
            self.near(side).start()

    def relay(self):
        for side in range(2):
            self.near(side).wait_recv()
            self.far(side).start()

    def arrive(self):
        for side in range(2):
            self.far(side).wait_recv()

    def sent(self):
        for side in range(2):
            self.near(side).wait_send()
            self.far(side).wait_send()


class Gather:
    def __init__(self, ring, shards, outs, layer, sems, local_sems):
        self.ring, self.shards, self.outs, self.layer, self.local_sems = ring, shards, outs, layer, local_sems
        side = ring.side
        self.ones, self.pairs = [], []
        for i in range(3):
            pair = [[] for _ in range(side)]
            for half in range(2):
                axis = 1 - half
                unit = 2 * i + half

                def owner(offset, axis=axis):
                    at = [ring.at[0], ring.at[1]]
                    at[axis] = ring.place(axis, offset)
                    return at[0] * side + at[1]

                self.ones.append(self.piece(i, half, axis, owner, self.region(shards[i], i, 0, half), sems, unit))
                for k in range(side):

                    def owner(offset, axis=axis, k=k):
                        at = [k, k]
                        at[1 - axis] = ring.place(1 - axis, offset)
                        return at[0] * side + at[1]

                    pair[k].append(self.piece(i, half, 1 - axis, owner, None, sems, 6 + unit * side + k))
            self.pairs += pair

    def piece(self, i, half, axis, owner, src, sems, number):
        out = self.outs[i].at[self.layer]
        return Piece(
            self.ring,
            axis,
            src,
            lambda offset: self.region(out, i, owner(offset), half),
            lambda offset, part: self.region(out, i, owner(offset), half, part),
            sems,
            number,
        )

    def region(self, ref, i, owner, half, part=None):
        rows, columns = self.shards[i].shape
        share = 2 if part is None else 4
        which = half if part is None else 2 * half + part
        if columns % (4 * LANES) == 0:
            first = owner * rows
            return ref.at[pl.ds(pl.multiple_of(first, 8), rows), pl.ds(which * (columns // share), columns // share)]
        length = rows // share
        return ref.at[pl.ds(pl.multiple_of(owner * rows + which * length, 8), length)]

    def local(self, i):
        rows = self.shards[i].shape[0]
        me = self.ring.at[0] * self.ring.side + self.ring.at[1]
        out = self.outs[i].at[self.layer, pl.ds(pl.multiple_of(me * rows, 8), rows)]
        return pltpu.make_async_copy(self.shards[i], out, self.local_sems.at[i])

    def start(self):
        for one in self.ones:
            one.start()
        for i in range(3):
            self.local(i).start()

    def relay(self):
        for one in self.ones:
            one.relay()

    def arrive(self):
        for one in self.ones:
            one.arrive()
        for i in range(3):
            self.local(i).wait()

    def finish(self):
        for pair in self.pairs:
            for piece in pair:
                piece.arrive()
        for one in (*self.ones, *(piece for pair in self.pairs for piece in pair)):
            one.sent()


def backward_kernel(side, wanted, gathered, h_hbm, dy_ref, *refs):
    wg_refs, wu_refs, wd_refs, refs = refs[:side], refs[side : 2 * side], refs[2 * side : 3 * side], refs[3 * side :]
    if gathered is not None:
        shards, refs = refs[:3], refs[3:]
    gg_ref, gu_ref, gd_ref, *refs = refs
    if wanted:
        h_ref, *refs = refs
    if gathered is not None:
        outs, refs = refs[:3], refs[3:]
    a_ref, at_ref, dyt_ref, hid_ref, dgate_ref, dup_ref, held_ref, local_sem, refs = *refs[:8], refs[8:]
    ga, gb, gd, ra, rb, rd, na, nb, nd, sa, sb, sd, refs = *refs[:12], refs[12:]
    ha, hb, hd, ra2, rb2, rd2, na2, nb2, nd2, sems, refs = *refs[:10], refs[10:]
    if wanted:
        da_ref, *refs = refs
    else:
        h_ref, *refs = refs
    tokens, d = dy_ref.shape
    size = tokens // CHUNKS
    t, steps = pl.program_id(0), pl.num_programs(0) - 1
    rows = gg_ref.shape[0]
    ring = Ring(side)
    half_d = hd.shape[2]
    first_a, first_b, first_d = (
        Scatter(ring, axis, g, r, n, sems.at[i]) for i, (axis, g, r, n) in enumerate(((0, ga, ra, na), (1, gb, rb, nb), (0, gd, rd, nd)))
    )
    second_a, second_b, second_d = (
        Scatter(ring, axis, g, r, n, sems.at[3 + i])
        for i, (axis, g, r, n) in enumerate(((1, ha, ra2, na2), (0, hb, rb2, nb2), (1, hd, rd2, nd2)))
    )

    if gathered is not None:
        others = Gather(ring, shards, outs, gathered, *refs)

    def beside(second):
        if gathered is None:
            return
        many = -(-len(others.pairs) // (pl.num_programs(0) - 2))
        for number, pair in enumerate(others.pairs):
            when, late = 1 + number // many, number % many >= (many + 1) // 2
            if late == second:

                @pl.when(t == when)
                def _(pair=pair):
                    for piece in pair:
                        piece.start()

                @pl.when(t == when + 1)
                def _(pair=pair):
                    for piece in pair:
                        piece.relay()

    @pl.when(t == 0)
    def _():
        ring.meet()
        if gathered is not None:
            others.start()
        copy = pltpu.make_async_copy(h_hbm, h_ref, local_sem)
        copy.start()
        copy.wait()
        @pl.loop(0, CHUNKS)
        def _(c):
            part = pl.ds(pl.multiple_of(c * size, size), size)
            a = normed(h_ref[part])
            a_ref[part] = a
            at_ref[:, part] = a.T
            dyt_ref[:, part] = dy_ref[part].T
            if wanted:
                da_ref[part] = jnp.zeros((size, d), F32)

    def joined(refs, axis):
        return jnp.concatenate([ref[0] for ref in refs], axis)

    def chunk(c):
        wg, wu, wd = joined(wg_refs, 1), joined(wu_refs, 1), joined(wd_refs, 0)
        part = pl.ds(pl.multiple_of(c * size, size), size)
        a = a_ref[part]
        gate, up = dot(a, wg), dot(a, wu)
        dhid = dot(dy_ref[part], wd, ((1,), (1,))).astype(BF16).astype(F32)
        s = jax.nn.sigmoid(gate)
        silu = gate * s
        hid_ref[part] = (silu * up).astype(BF16)
        dup = (dhid * silu).astype(BF16)
        dgate = (dhid * up * (s + silu * (1 - s))).astype(BF16)
        dup_ref[part] = dup
        dgate_ref[part] = dgate
        if wanted:
            by_both = jnp.concatenate([dgate, dup], 1)
            da_ref[part] += dot(by_both, jnp.concatenate([wg, wu], 1), ((1,), (1,)))

    def put(g, half):
        for place in range(side):
            ga[place, half] = g[side * rows * place : side * rows * (place + 1), :LANES].astype(BF16)
            mine = [g[rows * (side * x + place) : rows * (side * x + place + 1), LANES:] for x in range(side)]
            gb[place, half] = jnp.concatenate(mine, 0).astype(BF16)

    def own(total):
        return lambda place, half: total[half, pl.ds(pl.multiple_of(place * rows, 8), rows)]

    def mine(place, half):
        return sd[pl.ds(pl.multiple_of((2 * place + half) * half_d, 8), half_d)]

    def second_relay():
        second_a.relay(own(sa))
        second_b.relay(own(sb))

    def second_end(run):
        second_a.arrive()
        second_b.arrive()
        for two, total, tile in ((second_a, sa, 0), (second_b, sb, 1)):
            place = ring.place(two.axis, 0)
            for half, out in enumerate((gg_ref, gu_ref)):
                value = (own(total)(place, half) + two.received(half)).astype(BF16)
                for j in range(value.shape[1] // LANES):
                    lane = pl.multiple_of((run + steps * (tile + j)) * LANES, LANES)
                    out[:, pl.ds(lane, LANES)] = value[:, j * LANES : (j + 1) * LANES]

    computing, summing, ending = t < steps, t > 0, t > 1

    def stages():
        @pl.when(ending)
        def _():
            second_relay()

        @pl.when(summing)
        def _():
            for one in (first_a, first_b, first_d):
                one.relay()

        if gathered is not None:

            @pl.when(t == 1)
            def _():
                others.arrive()

        beside(False)

    @pl.loop(0, CHUNKS // 2)
    def _(i):
        @pl.when(computing)
        def _():
            chunk(2 * i)
            chunk(2 * i + 1)

        @pl.when(i == 0)
        def _():
            stages()

    @pl.when(computing)
    def _():
        g = dot(dyt_ref[...], hid_ref[...]).T.astype(BF16)
        held_ref[...] = g.reshape(held_ref.shape)

    if gathered is not None:

        @pl.when(t == 0)
        def _():
            others.relay()

    @pl.when(ending)
    def _():
        second_end(t - 2)

    @pl.when(summing)
    def _():
        for one in (first_a, first_b, first_d):
            one.arrive()
        for one, two, total in ((first_a, second_a, sa), (first_b, second_b, sb)):
            place = ring.place(one.axis, 0)
            for half in range(2):
                value = one.terms[place, half].astype(F32) + one.received(half)
                total[half] = value
                for p in range(side):
                    two.terms[p, half] = value[rows * p : rows * (p + 1)].astype(BF16)
                two.first(half).start()
        place = ring.place(0, 0)
        for half in range(2):
            value = gd[place, half].astype(F32) + first_d.received(half)
            count = value.shape[0]
            sd[pl.ds(pl.multiple_of((2 * (t - 1) + half) * count, count), count)] = value

    @pl.when(t == steps)
    def _():
        for p in range(side):
            for half in range(2):
                hd[p, half] = mine(p, half).astype(BF16)
        for half in range(2):
            second_d.first(half).start()

    @pl.when(computing)
    def _():
        gd[...] = held_ref[...]
        for half in range(2):
            first_d.first(half).start()

    beside(True)

    @pl.when(computing)
    def _():
        g = dot(at_ref[...], dgate_ref[...])
        put(g, 0)
        first_a.first(0).start()
        first_b.first(0).start()

    @pl.when(computing)
    def _():
        g = dot(at_ref[...], dup_ref[...])
        put(g, 1)
        first_a.first(1).start()
        first_b.first(1).start()

    if wanted:

        @pl.when(t == steps - 1)
        def _():
            @pl.loop(0, CHUNKS)
            def _(c):
                part = pl.ds(pl.multiple_of(c * size, size), size)
                wide = h_ref[part].astype(F32)
                by_a = da_ref[part].astype(BF16).astype(F32)
                scale = lax.rsqrt(jnp.mean(wide**2, -1, keepdims=True) + 1e-6)
                along = jnp.mean(by_a * wide, -1, keepdims=True)
                by_h = by_a * scale - wide * (along * scale * scale * scale)
                h_ref[part] = dy_ref[part] + by_h.astype(BF16)

    @pl.when(t == steps)
    def _():
        second_relay()
        second_d.relay(mine)
        second_end(t - 1)
        second_d.arrive()
        place = ring.place(1, 0)
        for half in range(2):
            gd_ref[half * half_d : (half + 1) * half_d] = (mine(place, half) + second_d.received(half)).astype(BF16)
        if gathered is not None:
            others.finish()


def backward(side, h, dy, wg, wu, wd, layer, wanted, shards=(), gathered=None):
    tokens, d = h.shape
    ff = wg.shape[2]
    tiles = ff // LANES
    steps = tiles // side
    rows, down_rows = d // side**2, ff // side**2
    width = side * LANES

    def tile(j):
        return lambda t: jnp.minimum(t, steps - 1) + steps * j

    across = [pl.BlockSpec((1, d, LANES), lambda t, j=j: (layer, 0, tile(j)(t))) for j in range(side)]
    down = [pl.BlockSpec((1, LANES, d), lambda t, j=j: (layer, tile(j)(t), 0)) for j in range(side)]
    shapes = [(side, 2, side * rows, LANES), (side, 2, side * rows, width - LANES), (side, 2, LANES // 2, d)]
    shapes2 = [(side, 2, rows, LANES), (side, 2, rows, width - LANES), (side, 2, down_rows // 2, d)]

    def buffers(shapes):
        terms = [pltpu.VMEM(s, BF16) for s in shapes]
        far = [pltpu.VMEM(s[1:], BF16) for s in shapes]
        near = [pltpu.VMEM((2, *s[1:]), BF16) for s in shapes]
        return terms + far + near

    totals = [
        pltpu.VMEM((2, side * rows, LANES), F32),
        pltpu.VMEM((2, side * rows, width - LANES), F32),
        pltpu.VMEM((side * down_rows, d), F32),
    ]
    scratch = [
        pltpu.VMEM((tokens, d), BF16),
        pltpu.VMEM((d, tokens), BF16),
        pltpu.VMEM((d, tokens), BF16),
        pltpu.VMEM((tokens, width), BF16),
        pltpu.VMEM((tokens, width), BF16),
        pltpu.VMEM((tokens, width), BF16),
        pltpu.VMEM(shapes[2], BF16),
        pltpu.SemaphoreType.DMA,
        *buffers(shapes),
        *totals,
        *buffers(shapes2),
        pltpu.SemaphoreType.DMA((6, 2, 4)),
    ]
    results = [(rows, ff), (rows, ff), (down_rows, d)] + [(tokens, d)] * wanted
    out_specs = [whole(s) for s in results]
    out_shape = [jax.ShapeDtypeStruct(s, BF16) for s in results]
    scratch.append(pltpu.VMEM((tokens, d), F32 if wanted else BF16))
    if shards:
        out_specs += [pl.BlockSpec(memory_space=pl.ANY)] * 3
        out_shape += [jax.ShapeDtypeStruct(w.shape, w.dtype) for w in (wg, wu, wd)]
        scratch += gather_scratch(side)
    return pl.pallas_call(
        functools.partial(backward_kernel, side, wanted, gathered),
        grid=(steps + 1,),
        in_specs=[pl.BlockSpec(memory_space=pl.ANY), whole((tokens, d)), *across, *across, *down, *(whole(s.shape) for s in shards)],
        out_specs=out_specs,
        out_shape=out_shape,
        scratch_shapes=scratch,
        cost_estimate=pl.CostEstimate(
            flops=2 * tokens * d * ff * (8 if wanted else 6), bytes_accessed=6 * 2 * d * ff, transcendentals=tokens * ff
        ),
        compiler_params=pltpu.CompilerParams(vmem_limit_bytes=63 * 2**20, collective_id=1 + layer, has_side_effects=True),
        name=f"backward_{layer}",
    )(h, dy, *[wg] * side, *[wu] * side, *[wd] * side, *shards)


def gather_kernel(side, layer, *refs):
    shards, outs, (sems, local_sems) = refs[:3], refs[6:9], refs[9:]
    ring = Ring(side)
    ring.meet()
    all_of = Gather(ring, shards, outs, layer, sems, local_sems)
    all_of.start()
    all_of.relay()
    all_of.arrive()
    for pair in all_of.pairs:
        for piece in pair:
            piece.start()
    for pair in all_of.pairs:
        for piece in pair:
            piece.relay()
    all_of.finish()


def gather_scratch(side):
    return [pltpu.SemaphoreType.DMA((2, 6 * (1 + side), 4)), pltpu.SemaphoreType.DMA((3,))]


def gather(side, layer, shards, weights):
    hbm = pl.BlockSpec(memory_space=pl.ANY)
    return pl.pallas_call(
        functools.partial(gather_kernel, side, layer),
        in_specs=[pl.BlockSpec(memory_space=pltpu.VMEM)] * 3 + [hbm] * 3,
        out_specs=[hbm] * 3,
        out_shape=[jax.ShapeDtypeStruct(w.shape, w.dtype) for w in weights],
        input_output_aliases={3: 0, 4: 1, 5: 2},
        scratch_shapes=gather_scratch(side),
        compiler_params=pltpu.CompilerParams(vmem_limit_bytes=60 * 2**20, collective_id=0, has_side_effects=True),
        name="gather",
    )(*shards, *weights)


def solution(mesh):
    side = math.isqrt(mesh.shape["dp"])

    def step(x, dy, *arrays):
        weights, ms, vs = (arrays[i : i + 3] for i in (0, 3, 6))
        x, dy = x[0], dy[0]
        layers = weights[0].shape[0]
        me = lax.axis_index("dp")

        states = [x]
        for n in range(layers - 1):
            states.append(forward(states[-1], *weights, n))

        def fresh(n):
            new = []
            for i in range(3):
                rows, columns = ms[i].shape[1:]
                w = lax.dynamic_slice(weights[i], (n, me * rows, 0), (1, rows, columns))[0]
                new.append(adamw(w.astype(F32), ms[i][n], vs[i][n], grads[n][i].astype(F32)))
            return new

        grads, shards = [None] * layers, ()
        for n in reversed(range(layers)):
            *out, = backward(side, states[n], dy, *weights, n, n > 0, shards, n + 1 if shards else None)
            grads[n], gathered = out[:3], out[-3:]
            dy = out[3]
            shards = fresh(n)
        gathered = gather(side, 0, shards, gathered)
        after = []
        for i in range(3):
            g = jnp.stack([grads[n][i] for n in range(layers)]).astype(F32)
            after.append(moments(ms[i], vs[i], g))
        return (*gathered, *(one[0] for one in after), *(one[1] for one in after))

    tokens, row = P(("rep", "dp"), None, None), P(None, "dp", None)
    return jax.shard_map(
        step,
        mesh=mesh,
        in_specs=(tokens,) * 2 + (P(),) * 3 + (row,) * 6,
        out_specs=(P("rep", None, None),) * 3 + (P("rep", "dp", None),) * 6,
        check_vma=False,
    )
```
